32 devices in a mesh: image: 4 (over y, x), band: 2 (over core), ga: 4 (over z).
Axes of the slice: x: 2, y: 2, z: 4, core: 2. Of those that a mesh axis runs over, the one named last changes fastest.
Arguments:
- wave_coeffs: bfloat16 [4, 64, 2, 262144], P('image', 'band', None, 'ga'), may hold values from -6 to 6
- occupation: float32 [4, 64], P('image', 'band'), may hold values from 0.003125 to 0.0625
- form_factor: float32 [4, 8, 262144], P(None, None, 'ga'), may hold values from -0.005859375 to 0.005859375
- g_vectors: float32 [3, 262144], P(None, 'ga'), may hold values from -2 to 2
- species: int32 [64], replicated, may hold values from 0 to 3
- proj_count: int32 [4], replicated, may hold values from 1 to 8, as said below
- coupling: float32 [4, 8], replicated, may hold values from 0.5 to 2.5
- positions: float32 [4, 3, 64], P('image'), may hold values from -5.4 to 29.4, as said below
- energy_rest: float32 [4], P('image'), may hold values from -8 to 8
- force_rest: float32 [4, 3, 64], P('image'), may hold values from -6 to 6
- end_positions: float32 [2, 3, 64], replicated, may hold values from -5.4 to 29.4, as said below
- end_energy: float32 [2], replicated, may hold values from -8 to 8
- climb_index: int32 [1], replicated, may hold values from 0 to 3
- tangent_kind: int32 [4], P('image'), may hold values from 0 to 3
Outputs:
- neb_force: float32 [4, 3, 64], P('image')
- energy: float32 [4], P('image')
The draws below stay inside these ranges and needn't reach their ends.
Inputs may be any that keep to these rules, and one draw needn't show every extreme that they name: `proj_count`: each species has between 1 and 8 live projector slots, and some species has exactly 8. `positions`: atom coordinates in bohr. `end_positions`: atom coordinates in bohr.
All inputs are finite; a program needn't handle non-finite values.
Results may differ from the reference program's by a relative error of at most 0.0003.
The reference program's roundings to bfloat16 on the way (of `projector` and `stacked`) count: a program that leaves them out, or rounds other values in their place, can miss the bound.
Values sent between devices are 32-bit elements; how exact they have to be, the bound alone decides.
A program may use at most 128 MiB of HBM per device.

```python
import jax
import jax.numpy as jnp
from jax import lax

NG = 262144
ATOMS = 64
PMAX = 8
SPECIES = 4
IMG = 4
BANDS = 64
N_GA = 4


def chain_path(key):
    base_key = jax.random.fold_in(key, 11)
    step_key = jax.random.fold_in(key, 12)
    base = jax.random.uniform(base_key, (3, ATOMS), jnp.float32, 0.0, 24.0)
    steps = 0.3 * jnp.clip(jax.random.normal(step_key, (IMG + 2, 3, ATOMS), jnp.float32), -3.0, 3.0)
    return base[None, :, :] + jnp.cumsum(steps, axis=0)


def draw_positions(key, part):
    return chain_path(key)[1:IMG + 1]


def draw_end_positions(key, part):
    path = chain_path(key)
    return jnp.stack([path[0], path[IMG + 1]], axis=0)


def draw_proj_count(key, part):
    counts = jax.random.randint(jax.random.fold_in(key, 21), (SPECIES,), 1, PMAX + 1, jnp.int32)
    filled = jax.random.randint(jax.random.fold_in(key, 22), (), 0, SPECIES, jnp.int32)
    return jnp.where(jnp.arange(SPECIES, dtype=jnp.int32) == filled, PMAX, counts).astype(jnp.int32)


def place_ends(drawn, rng, smallest, high):
    shape = drawn.shape
    spot = [jax.random.randint(jax.random.fold_in(rng, axis), (), 0, shape[axis]) for axis in range(len(shape))]
    drawn = drawn.at[tuple(spot)].set(smallest)
    longest = shape.index(max(shape))
    spot[longest] = (spot[longest] + 1) % shape[longest]
    return drawn.at[tuple(spot)].set(high)


def levels(stream_key, extent, cuts, low, top_value):
    loudness = 1.0
    for dim, blocks in cuts:
        steps = jax.random.uniform(jax.random.fold_in(jax.random.fold_in(stream_key, 6), dim), (blocks,), jnp.float32, low / len(cuts), top_value / len(cuts))
        loudness = loudness * jnp.repeat(jnp.exp(steps), extent[dim] // blocks).reshape((-1,) + (1,) * (len(extent) - 1 - dim))
    return loudness


def centred(stream_key, dims, deviation, limit, cuts=(), kind=jnp.bfloat16):
    array = jax.random.normal(stream_key, dims, jnp.float32) * deviation
    if len(cuts) > 0:
        array = levels(stream_key, dims, cuts, -0.22, 0.18) * array
    return jnp.clip(array, min=-limit, max=limit).astype(kind)


def setup_inputs(seed: int = 0) -> dict:
    key_of = jax.random.split(jax.random.key(seed), 15)
    return {
        "wave_coeffs": centred(key_of[0], (IMG, BANDS, 2, NG), 1.0, 6.0, ((0, 4), (1, 2), (3, 4))),
        "occupation": jnp.clip(0.003125 + 0.059375 * jax.random.uniform(key_of[1], (IMG, BANDS), jnp.float32) ** levels(key_of[1], (IMG, BANDS), ((0, 4), (1, 2)), -0.2, 0.2), 0.003125, 0.0625),
        "form_factor": centred(key_of[2], (SPECIES, PMAX, NG), (4 * NG) ** -0.5, 0.005859375, ((2, 4),), jnp.float32),
        "g_vectors": jnp.clip(jax.random.uniform(key_of[3], (3, NG), jnp.float32, -2.0, 2.0) * levels(key_of[3], (3, NG), ((1, 4),), -0.4, 0.0), -2.0, 2.0),
        "species": place_ends(jax.random.randint(key_of[4], (ATOMS,), 0, SPECIES), jax.random.fold_in(key_of[4], 1), 0, SPECIES - 1).astype(jnp.int32),
        "proj_count": draw_proj_count(jax.random.fold_in(key_of[14], 71), 0),
        "coupling": jnp.clip(jax.random.uniform(key_of[6], (SPECIES, PMAX), jnp.float32, 0.5, 2.5), 0.5, 2.5),
        "positions": draw_positions(jax.random.fold_in(key_of[14], 71), 0),
        "energy_rest": centred(key_of[8], (IMG,), 2.0, 8.0, ((0, 4),), jnp.float32),
        "force_rest": centred(key_of[9], (IMG, 3, ATOMS), 1.0, 6.0, ((0, 4),), jnp.float32),
        "end_positions": draw_end_positions(jax.random.fold_in(key_of[14], 71), 0),
        "end_energy": centred(key_of[11], (2,), 2.0, 8.0, (), jnp.float32),
        "climb_index": jax.random.randint(key_of[12], (1,), 0, IMG).astype(jnp.int32),
        "tangent_kind": place_ends(jax.random.randint(key_of[13], (IMG,), 0, 4), jax.random.fold_in(key_of[13], 1), 0, 3).astype(jnp.int32),
    }


spring_constant = 5.0

def atom_tables(species, proj_count, coupling):
    is_species = (species[:, None] == jnp.arange(SPECIES)[None, :]).astype(jnp.float32)
    is_live = (jnp.arange(PMAX)[None, :] < proj_count[:, None]).astype(jnp.float32)
    species_mask = is_species[:, :, None] * is_live[None, :, :]
    strength = lax.optimization_barrier(jnp.sum(species_mask * coupling[None, :, :], axis=1))
    return (species_mask, strength)

def projectors(atom_pos, species_mask, form_factor, g_vectors):
    phases = atom_pos[0][:, None] * g_vectors[0][None, :]
    phases = phases + atom_pos[1][:, None] * g_vectors[1][None, :]
    phases = phases + atom_pos[2][:, None] * g_vectors[2][None, :]
    cosine = jnp.cos(phases)
    sine_part = jnp.sin(phases)
    radial = species_mask[:, 0, :, None] * form_factor[0][None, :, :]
    for spec_num in range(1, SPECIES):
        radial = radial + species_mask[:, spec_num, :, None] * form_factor[spec_num][None, :, :]
    real_part = radial * cosine[:, None, :]
    imag_part = -radial * sine_part[:, None, :]
    joined = jnp.concatenate([real_part, imag_part], axis=-1).astype(jnp.bfloat16)
    return joined.reshape(joined.shape[0] * joined.shape[1], joined.shape[2])

def stack_waves(waves_here, g_vectors):
    band_count = waves_here.shape[0]
    real_part = waves_here[:, 0, :].astype(jnp.float32)
    imag_part = waves_here[:, 1, :].astype(jnp.float32)
    pieces = [waves_here.reshape(band_count, 2 * waves_here.shape[2])]
    for axis_num in range(3):
        direction = g_vectors[axis_num][None, :]
        pieces.append(jnp.concatenate([-direction * imag_part, direction * real_part], axis=-1).astype(jnp.bfloat16))
    return jnp.concatenate(pieces, axis=0)

def contract(projector, stacked):
    return 2.0 * lax.dot_general(projector, stacked, (((1,), (1,)), ((), ())), preferred_element_type=jnp.float32)

def nonlocal_terms(proj_sums, occupied, strength):
    band_count = occupied.shape[0]
    atom_count = strength.shape[0]
    intersect = proj_sums[:, :band_count]
    weighted = intersect * occupied[None, :]
    energy_part = jnp.sum(strength.reshape(-1) * lax.optimization_barrier(jnp.sum(weighted * intersect, axis=1)))
    forces = []
    for axis_num in range(3):
        slope = proj_sums[:, (axis_num + 1) * band_count:(axis_num + 2) * band_count]
        per_row = lax.optimization_barrier(jnp.sum(weighted * slope, axis=1)).reshape(atom_count, PMAX)
        forces.append(-2.0 * lax.optimization_barrier(jnp.sum(strength * per_row, axis=1)))
    return (energy_part, jnp.stack(forces, axis=0))

def neb_project(force, here, prev_pos, next_pos, energy, prev_energy, next_energy, tangent_kind, is_climb):
    to_next = next_pos - here
    from_prev = here - prev_pos
    rise_next = jnp.abs(next_energy - energy)
    rise_prev = jnp.abs(prev_energy - energy)
    larger = jnp.maximum(rise_next, rise_prev)
    smaller = jnp.minimum(rise_next, rise_prev)
    rising = next_energy > prev_energy
    weight_next = 1.0 + jnp.where(rising, larger, smaller)
    weight_prev = 1.0 + jnp.where(rising, smaller, larger)
    stiff_next = spring_constant * (1.0 + jax.nn.sigmoid(0.5 * (next_energy + energy)))
    stiff_prev = spring_constant * (1.0 + jax.nn.sigmoid(0.5 * (prev_energy + energy)))
    length_next = jnp.sqrt(lax.optimization_barrier(jnp.sum(to_next * to_next, axis=(1, 2))) + 1.0)
    length_prev = jnp.sqrt(lax.optimization_barrier(jnp.sum(from_prev * from_prev, axis=(1, 2))) + 1.0)
    upwind = weight_next[:, None, None] * to_next + weight_prev[:, None, None] * from_prev
    forward = to_next / length_next[:, None, None]
    backward = from_prev / length_prev[:, None, None]
    kind = tangent_kind[:, None, None]
    tangent = jnp.where(kind == 0, upwind, jnp.where(kind == 1, forward + backward, jnp.where(kind == 2, forward, backward)))
    unit_tangent = tangent / jnp.sqrt(lax.optimization_barrier(jnp.sum(tangent * tangent, axis=(1, 2))) + 1.0)[:, None, None]
    along = lax.optimization_barrier(jnp.sum(force * unit_tangent, axis=(1, 2)))[:, None, None]
    climbing = force - 2.0 * along * unit_tangent
    regular = force - along * unit_tangent + (stiff_next * length_next - stiff_prev * length_prev)[:, None, None] * unit_tangent
    return jnp.where(is_climb[:, None, None], climbing, regular)

def reference(wave_coeffs, occupation, form_factor, g_vectors, species, proj_count, coupling, positions, energy_rest, force_rest, end_positions, end_energy, climb_index, tangent_kind):
    species_mask, strength = atom_tables(species, proj_count, coupling)
    block_len = NG // N_GA
    energies = []
    forces = []
    for image_num in range(IMG):
        waves_image = wave_coeffs[image_num]
        atom_pos = positions[image_num]

        def accumulate(block_num, total):
            start = (block_num * block_len).astype(jnp.int32)
            waves_block = lax.dynamic_slice_in_dim(waves_image, start, block_len, 2)
            form_block = lax.dynamic_slice_in_dim(form_factor, start, block_len, 2)
            g_block = lax.dynamic_slice_in_dim(g_vectors, start, block_len, 1)
            stacked = stack_waves(waves_block, g_block)
            projector = projectors(atom_pos, species_mask, form_block, g_block)
            return total + contract(projector, stacked)
        initial = jnp.zeros((ATOMS * PMAX, 4 * BANDS), jnp.float32)
        proj_sums = lax.fori_loop(0, N_GA, accumulate, initial)
        energy_part, force_part = nonlocal_terms(proj_sums, occupation[image_num], strength)
        energies.append(energy_part)
        forces.append(force_part)
    energy = energy_rest + jnp.stack(energies)
    force = force_rest + jnp.stack(forces, axis=0)
    chain_pos = jnp.concatenate([end_positions[:1], positions, end_positions[1:]], axis=0)
    chain_energy = jnp.concatenate([end_energy[:1], energy, end_energy[1:]], axis=0)
    is_climb = jnp.arange(IMG, dtype=jnp.int32) == climb_index[0]
    neb_force = neb_project(force, positions, chain_pos[:-2], chain_pos[2:], energy, chain_energy[:-2], chain_energy[2:], tangent_kind, is_climb)
    return (neb_force, energy)
```

```python
import functools

import jax
import jax.numpy as jnp
from jax import lax
from jax.experimental import pallas as pl
from jax.experimental.pallas import tpu as pltpu
from jax.sharding import PartitionSpec as P

SPRING = 5.0
SIN_HALF = (0.7071067780965931, -0.02946276693049568, 0.00036827213876565137, -2.1885830267998076e-06, 7.194201360627222e-09)
COS_HALF = (-1.4142134949348355, 0.17677635430234293, -0.003682571658574129, 3.061195661905538e-05, -1.2786908538293617e-07)
TURN_HIGH = 6.28125
TURN_LOW = 0.001935307179586232
ROUNDER = 12582912.0
LANE = 128
WIDE = 256
CHUNKS = 8
MESH = pl.DeviceIdType.MESH
F32 = jnp.float32
BF16 = jnp.bfloat16


def horner(coefs, z):
    total = coefs[-1] * z + coefs[-2]
    for coef in coefs[-3::-1]:
        total = total * z + coef
    return total


def cos_and_minus_sin(phases):
    turns = (phases * 0.15915494309189535 + ROUNDER) - ROUNDER
    r = (phases - turns * TURN_HIGH) - turns * TURN_LOW
    z = r * r
    half_sin = r * horner(SIN_HALF, z)
    return (1.0 - half_sin * half_sin, half_sin * horner(COS_HALF, z))


def iota(shape, dim):
    return lax.broadcasted_iota(jnp.int32, shape, dim)


def column(row, start, rows):
    n = row.shape[1]
    here = iota((rows, n), 1) == iota((rows, n), 0) + start
    return jnp.sum(jnp.where(here, row, 0.0), axis=1, keepdims=True)


def row_of(col, start):
    rows = col.shape[0]
    here = iota((rows, LANE), 1) == iota((rows, LANE), 0) + start
    return jnp.sum(jnp.where(here, col, 0.0), axis=0, keepdims=True)


def total(x):
    return jnp.sum(jnp.sum(x, axis=1, keepdims=True), axis=0, keepdims=True)


def kernel(
    w_hbm, occ_hbm, ff_hbm, g_hbm, spec_hbm, count_hbm, coup_hbm, pos_hbm, erest_hbm, frest_hbm,
    endp_hbm, ende_hbm, climb_hbm, kind_hbm,
    force_out, energy_out,
    raw_other, raw_own, w_send, w_all, ff, g, pos, coup, occ, erest, frest, endp, ende,
    spec, count, climb, kind,
    pos_wide, live, strength, occ_part, occ_peer, trig_a, trig_b, rad_a, rad_b,
    part, part_peer, z_send, z_recv, msg, msgs,
    small_sem, other_sem, own_sem, ff_sem, g_sem, w_send_sem, w_recv_sem, occ_sem,
    part_sems, z_sems, msg_send_sem, msg_recv_sem,
):
    image, band, ga = (lax.axis_index(a) for a in ("image", "band", "ga"))
    n_image, n_band, n_ga = (lax.axis_size(a) for a in ("image", "band", "ga"))
    group = n_band * n_ga
    side = lax.rem(band, 2)
    peer = band + 1 - 2 * side
    bands = w_hbm.shape[0]
    blocks, tiles = raw_own.shape[0], raw_own.shape[1]
    species, slots = coup.shape
    atoms = pos.shape[2]
    half_len = ff.shape[2]
    n_wide = half_len // WIDE
    step_tiles = tiles // CHUNKS
    owners = part.shape[0]
    own_atoms = atoms // owners
    own_rows = part.shape[1]
    n_groups = atoms // 8

    small = [
        (occ_hbm, occ), (coup_hbm, coup), (pos_hbm, pos), (erest_hbm, erest), (frest_hbm, frest), (endp_hbm, endp),
        (ende_hbm, ende), (spec_hbm, spec), (count_hbm, count), (climb_hbm, climb), (kind_hbm, kind),
    ]
    small = [pltpu.make_async_copy(a, b, small_sem.at[i]) for i, (a, b) in enumerate(small)]

    def wave_copies(raw, which, c, count, sem):
        at = which * tiles + c * count
        return [
            pltpu.make_async_copy(
                w_hbm.at[n, pl.ds(at, count)],
                raw.at[n // 8, pl.ds(c * count, count), pl.ds(2 * (n % 8), 2), :],
                sem,
            )
            for n in range(bands)
        ]

    def start_other(c):
        for copy in wave_copies(raw_other, 1 - side, c, step_tiles, other_sem.at[c]):
            copy.start()

    mine = pl.ds(pl.multiple_of(side * half_len, WIDE), half_len)
    ff_copy = pltpu.make_async_copy(ff_hbm.at[:, :, mine], ff, ff_sem)
    g_copy = pltpu.make_async_copy(g_hbm.at[:, mine], g, g_sem)
    start_other(0)
    for copy in small:
        copy.start()
    start_other(1)

    barrier = pltpu.get_barrier_semaphore()
    for d_image in (0, 1, n_image - 1):
        for d_band in range(n_band):
            for d_ga in range(n_ga):
                if (d_image, d_band, d_ga) != (0, 0, 0):
                    there = (
                        lax.rem(image + d_image, n_image), lax.rem(band + d_band, n_band), lax.rem(ga + d_ga, n_ga)
                    )
                    pl.semaphore_signal(barrier, inc=1, device_id=there, device_id_type=MESH)

    for c in range(2, CHUNKS):
        start_other(c)
    g_copy.start()
    own_copies = wave_copies(raw_own, side, 0, tiles, own_sem)
    for copy in own_copies:
        copy.start()
    ff_copy.start()

    for copy in small:
        copy.wait()
    for c in range(3):
        for j in range(n_groups):
            pos_wide[c, 8 * j : 8 * j + 8, :] = jnp.broadcast_to(column(pos[0, c : c + 1, :], 8 * j, 8), (8, LANE))
    for s in range(species):
        alive = (iota((slots, LANE), 0) < count[s]).astype(F32)
        live[s] = alive
        strength[s] = alive * column(coup[s : s + 1, :], 0, slots)
    lanes = iota((1, LANE), 1)
    here = lax.rem(lanes // bands, 2) == side
    occ_part[...] = jnp.broadcast_to(jnp.where(here, jnp.concatenate([occ[...]] * (LANE // bands), axis=1), 0.0), (8, LANE))

    def wave_push(c):
        at = pl.ds(c * step_tiles, step_tiles)
        return pltpu.make_async_remote_copy(
            src_ref=w_send.at[:, at], dst_ref=w_all.at[side, :, at],
            send_sem=w_send_sem.at[c], recv_sem=w_recv_sem.at[c],
            device_id={"band": peer}, device_id_type=MESH,
        )

    def wave_arrival(c):
        at = pl.ds(c * step_tiles, step_tiles)
        return pltpu.make_async_remote_copy(
            src_ref=w_send.at[:, at], dst_ref=w_all.at[1 - side, :, at],
            send_sem=w_send_sem.at[c], recv_sem=w_recv_sem.at[c],
            device_id={"band": peer}, device_id_type=MESH,
        )

    occ_push = pltpu.make_async_remote_copy(
        src_ref=occ_part, dst_ref=occ_peer, send_sem=occ_sem.at[0], recv_sem=occ_sem.at[1],
        device_id={"band": peer}, device_id_type=MESH,
    )

    def widen_other(c):
        def one(t, carry):
            at = c * step_tiles + t
            for b in range(blocks):
                w_send[b, at] = raw_other[b, at].astype(F32)
            return carry

        lax.fori_loop(0, step_tiles, one, 0, unroll=8)

    for c in range(CHUNKS):
        for copy in wave_copies(raw_other, 1 - side, c, step_tiles, other_sem.at[c]):
            copy.wait()
        widen_other(c)
        if c == 0:
            pl.semaphore_wait(barrier, 3 * group - 1)
        wave_push(c).start()
    occ_push.start()

    for copy in own_copies:
        copy.wait()

    def widen_own(t, carry):
        for b in range(blocks):
            w_all[side, b, t] = raw_own[b, t].astype(F32)
        return carry

    lax.fori_loop(0, tiles, widen_own, 0, unroll=8)
    g_copy.wait()
    ff_copy.wait()

    def g_rows(at):
        return [jnp.broadcast_to(g[c : c + 1, at], (8, WIDE)) for c in range(3)]

    def doubled(x):
        return jnp.concatenate([x] * (WIDE // LANE), axis=1)

    def prepare(k, trig, rad):
        at = pl.ds(pl.multiple_of(k * WIDE, WIDE), WIDE)
        for s in range(species):
            rad[s] = ff[s, :, at] * doubled(live[s])
        gs = g_rows(at)
        for j in range(n_groups):
            rows = slice(8 * j, 8 * j + 8)
            phases = doubled(pos_wide[0, rows, :]) * gs[0]
            phases = phases + doubled(pos_wide[1, rows, :]) * gs[1]
            phases = phases + doubled(pos_wide[2, rows, :]) * gs[2]
            cosine, minus_sine = cos_and_minus_sin(phases)
            trig[j, 0] = cosine
            trig[j, 1] = minus_sine

    def stage(k):
        at = pl.ds(pl.multiple_of(k * WIDE, WIDE), WIDE)
        gs = g_rows(at)

        def rows(uv):
            pieces = []
            for s in range(2):
                for b in range(blocks):
                    pieces.append(jnp.concatenate(
                        [w_all[s, b, 2 * k + t, pl.ds(uv, 8, stride=2), :] for t in range(WIDE // LANE)], axis=1))
            return pieces

        u, v = rows(0), rows(1)
        real = list(u)
        imag = list(v)
        for c in range(3):
            minus = -gs[c]
            real += [minus * x for x in v]
            imag += [gs[c] * x for x in u]
        pltpu.matmul_push_rhs(jnp.concatenate(real, axis=0).astype(BF16), 0, 0, transpose=True)
        pltpu.matmul_push_rhs(jnp.concatenate(imag, axis=0).astype(BF16), 0, 1, transpose=True)

    def multiply(trig, rad, accs, j):
        radial = [rad[spec[8 * j + i]] for i in range(8)]
        for q in range(2):
            lhs = jnp.concatenate([radial[i] * trig[j, q, i : i + 1, :] for i in range(8)], axis=0).astype(BF16)
            pltpu.matmul_acc_lhs(accs[q][j], lhs, load_staged_rhs=0 if j == 0 else None)

    def with_accumulators(*refs):
        accs = (refs[:n_groups], refs[n_groups:])
        for ref in refs:
            pltpu.matmul_pop(ref)

        def wide_tile(k, now, later):
            after = jnp.minimum(k + 1, n_wide - 1)
            multiply(*now, accs, 0)
            stage(after)
            prepare(after, *later)
            for j in range(1, n_groups):
                multiply(*now, accs, j)

        wave_arrival(0).wait_recv()
        prepare(0, trig_a, rad_a)
        stage(0)
        per_chunk = n_wide // CHUNKS

        def pair(i, carry):
            k = 2 * i

            @pl.when((lax.rem(k + 2, per_chunk) == 0) & (k + 2 < n_wide))
            def _():
                wave_arrival((k + 2) // per_chunk).wait_recv()

            wide_tile(k, (trig_a, rad_a), (trig_b, rad_b))
            wide_tile(k + 1, (trig_b, rad_b), (trig_a, rad_a))
            return carry

        lax.fori_loop(0, n_wide // 2, pair, 0)
        for j in range(n_groups):
            sums = 2.0 * (pltpu.matmul_pop(accs[0][j]) + pltpu.matmul_pop(accs[1][j]))
            for i in range(8 // own_atoms):
                part[j * (8 // own_atoms) + i] = sums[i * own_rows : (i + 1) * own_rows]
        zeros = jnp.zeros((8 * slots, WIDE), BF16)
        for q in range(2):
            pltpu.matmul_acc_lhs(accs[q][0], zeros, load_staged_rhs=0)
            pltpu.matmul_pop(accs[q][0])

    pl.run_scoped(
        with_accumulators,
        *[pltpu.ACC(q)((8 * slots, WIDE), F32) for q in range(2) for _ in range(n_groups)],
    )

    def pair_push(q):
        return pltpu.make_async_remote_copy(
            src_ref=part.at[(1 - side) * n_ga + q], dst_ref=part_peer.at[q],
            send_sem=part_sems.at[0, q], recv_sem=part_sems.at[1, q],
            device_id={"band": peer}, device_id_type=MESH,
        )

    def z_push(d):
        return pltpu.make_async_remote_copy(
            src_ref=z_send.at[d - 1], dst_ref=z_recv.at[d - 1],
            send_sem=z_sems.at[0, d - 1], recv_sem=z_sems.at[1, d - 1],
            device_id={"ga": lax.rem(ga + d, n_ga)}, device_id_type=MESH,
        )

    order = list(range(1, n_ga)) + [0]
    for d in order:
        pair_push(lax.rem(ga + d, n_ga)).start()
    for d in order[:-1]:
        q = lax.rem(ga + d, n_ga)
        pair_push(q).wait_recv()
        z_send[d - 1] = part[side * n_ga + q] + part_peer[q]
        z_push(d).start()
    pair_push(ga).wait_recv()
    occ_push.wait()
    weights = occ_part[0:1, :] + occ_peer[0:1, :]
    sums = part[side * n_ga + ga] + part_peer[ga]
    for d in range(1, n_ga):
        z_push(d).wait_recv()
        sums = sums + z_recv[d - 1]

    owner = side * n_ga + ga
    first = owner * own_atoms
    low = iota((slots, LANE), 1) < LANE // 2
    rows_0, rows_1 = [], []
    for i in range(own_atoms):
        rows = slice(i * slots, (i + 1) * slots)
        left, right = sums[rows, :LANE], sums[rows, LANE:]
        becp = jnp.where(low, left, pltpu.roll(left, LANE // 2, 1))
        weighted = becp * weights * strength[spec[first + i]]
        rows_0.append(jnp.sum(weighted * left, axis=0, keepdims=True))
        rows_1.append(jnp.sum(weighted * right, axis=0, keepdims=True))
    rows_0, rows_1 = jnp.concatenate(rows_0, axis=0), jnp.concatenate(rows_1, axis=0)
    low = iota((own_atoms, LANE), 1) < LANE // 2
    cols = [
        jnp.sum(jnp.where(low == is_low, x, 0.0), axis=1, keepdims=True)
        for x, is_low in ((rows_0, True), (rows_0, False), (rows_1, True), (rows_1, False))
    ]
    energy_part = jnp.broadcast_to(jnp.sum(cols[0], axis=0, keepdims=True), (1, LANE))
    force_part = [-2.0 * row_of(col, first) for col in cols[1:]]

    def padded(x):
        return jnp.concatenate([x, jnp.zeros((x.shape[0], LANE - x.shape[1]), F32)], axis=1)

    rest = jnp.full((1, LANE), erest[0], F32)
    here_pos = padded(pos[0])
    message = jnp.concatenate([energy_part] + force_part + [rest, here_pos], axis=0)
    msg[...] = message
    slot = band * n_ga + ga
    msgs[1, slot] = message

    pushes = []
    count_pushes = 0
    for place, d_image in ((1, 0), (0, 1), (2, n_image - 1)):
        for d_band in range(n_band):
            for d_ga in range(n_ga):
                if (d_image, d_band, d_ga) != (0, 0, 0):
                    there = (
                        lax.rem(image + d_image, n_image), lax.rem(band + d_band, n_band), lax.rem(ga + d_ga, n_ga)
                    )
                    push = pltpu.make_async_remote_copy(
                        src_ref=msg, dst_ref=msgs.at[place, slot],
                        send_sem=msg_send_sem.at[count_pushes], recv_sem=msg_recv_sem.at[place, slot],
                        device_id=there, device_id_type=MESH,
                    )
                    push.start()
                    pushes.append(push)
                    count_pushes += 1
    for place, d_image in ((1, 0), (0, 1), (2, n_image - 1)):
        for d_band in range(n_band):
            for d_ga in range(n_ga):
                if (d_image, d_band, d_ga) != (0, 0, 0):
                    sender = lax.rem(band + d_band, n_band) * n_ga + lax.rem(ga + d_ga, n_ga)
                    pltpu.make_async_remote_copy(
                        src_ref=msg, dst_ref=msgs.at[place, sender],
                        send_sem=msg_send_sem.at[0], recv_sem=msg_recv_sem.at[place, sender],
                        device_id=(image, peer, ga), device_id_type=MESH,
                    ).wait_recv()

    def gathered(place):
        out = msgs[place, 0]
        first_msg = out
        for s in range(1, group):
            out = out + msgs[place, s]
        return first_msg[4:5, 0:1] + out[0:1, 0:1], out[1:4, :], first_msg[5:8, :]

    energy, force_nl, _ = gathered(1)
    prev_energy, _, prev_pos = gathered(0)
    next_energy, _, next_pos = gathered(2)
    ends = [padded(endp[s]) for s in range(2)]
    at_start, at_end = image == 0, image == n_image - 1
    prev_pos = jnp.where(jnp.full((3, LANE), at_start), ends[0], prev_pos)
    next_pos = jnp.where(jnp.full((3, LANE), at_end), ends[1], next_pos)
    prev_energy = jnp.where(jnp.full((1, 1), at_start), jnp.full((1, 1), ende[0], F32), prev_energy)
    next_energy = jnp.where(jnp.full((1, 1), at_end), jnp.full((1, 1), ende[1], F32), next_energy)
    force = padded(frest[0]) + force_nl

    to_next = next_pos - here_pos
    from_prev = here_pos - prev_pos
    rise_next = jnp.abs(next_energy - energy)
    rise_prev = jnp.abs(prev_energy - energy)
    larger = jnp.maximum(rise_next, rise_prev)
    smaller = jnp.minimum(rise_next, rise_prev)
    rising = next_energy > prev_energy
    weight_next = 1.0 + jnp.where(rising, larger, smaller)
    weight_prev = 1.0 + jnp.where(rising, smaller, larger)
    stiff_next = SPRING * (1.0 + 1.0 / (1.0 + jnp.exp(-0.5 * (next_energy + energy))))
    stiff_prev = SPRING * (1.0 + 1.0 / (1.0 + jnp.exp(-0.5 * (prev_energy + energy))))
    length_next = jnp.sqrt(total(to_next * to_next) + 1.0)
    length_prev = jnp.sqrt(total(from_prev * from_prev) + 1.0)
    upwind = weight_next * to_next + weight_prev * from_prev
    forward = to_next / length_next
    backward = from_prev / length_prev
    rule = jnp.full((3, LANE), kind[0], jnp.int32)
    tangent = jnp.where(
        rule == 0, upwind, jnp.where(rule == 1, forward + backward, jnp.where(rule == 2, forward, backward))
    )
    unit = tangent / jnp.sqrt(total(tangent * tangent) + 1.0)
    along = total(force * unit)
    climbing = force - 2.0 * along * unit
    regular = force - along * unit + (stiff_next * length_next - stiff_prev * length_prev) * unit
    is_climb = jnp.full((3, LANE), climb[0], jnp.int32) == image
    result = jnp.where(is_climb, climbing, regular)
    force_out[0] = result[:, :atoms]
    energy_out[0] = jnp.sum(energy)

    for c in range(CHUNKS):
        wave_push(c).wait_send()
    for d in order:
        pair_push(lax.rem(ga + d, n_ga)).wait_send()
    for d in range(1, n_ga):
        z_push(d).wait_send()
    for push in pushes:
        push.wait_send()


def per_device(
    wave_coeffs, occupation, form_factor, g_vectors, species, proj_count, coupling, positions, energy_rest,
    force_rest, end_positions, end_energy, climb_index, tangent_kind,
):
    _, bands, _, length = wave_coeffs.shape
    kinds, slots, _ = form_factor.shape
    atoms = species.shape[0]
    n_band, n_ga = lax.axis_size("band"), lax.axis_size("ga")
    waves = wave_coeffs[0].reshape(bands, 2, length // LANE, LANE).transpose(0, 2, 1, 3)
    blocks = bands // 8
    tiles = length // (2 * LANE)
    half_len = length // 2
    owners = 2 * n_ga
    own_rows = atoms * slots // owners
    group = n_band * n_ga
    args = (
        waves, occupation, form_factor, g_vectors, species, proj_count, coupling, positions, energy_rest,
        force_rest, end_positions, end_energy, climb_index, tangent_kind,
    )
    vmem, smem, dma = pltpu.VMEM, pltpu.SMEM, pltpu.SemaphoreType.DMA
    return pl.pallas_call(
        kernel,
        in_specs=[pl.BlockSpec(memory_space=pl.ANY)] * len(args),
        out_specs=[pl.BlockSpec(memory_space=pltpu.VMEM), pl.BlockSpec(memory_space=pltpu.SMEM)],
        out_shape=[jax.ShapeDtypeStruct(force_rest.shape, F32), jax.ShapeDtypeStruct(energy_rest.shape, F32)],
        scratch_shapes=[
            vmem((blocks, tiles, 16, LANE), BF16),
            vmem((blocks, tiles, 16, LANE), BF16),
            vmem((blocks, tiles, 16, LANE), F32),
            vmem((2, blocks, tiles, 16, LANE), F32),
            vmem((kinds, slots, half_len), F32),
            vmem((3, half_len), F32),
            vmem(positions.shape, F32),
            vmem(coupling.shape, F32),
            vmem(occupation.shape, F32),
            smem(energy_rest.shape, F32),
            vmem(force_rest.shape, F32),
            vmem(end_positions.shape, F32),
            smem(end_energy.shape, F32),
            smem(species.shape, jnp.int32),
            smem(proj_count.shape, jnp.int32),
            smem(climb_index.shape, jnp.int32),
            smem(tangent_kind.shape, jnp.int32),
            vmem((3, atoms, LANE), F32),
            vmem((kinds, slots, LANE), F32),
            vmem((kinds, slots, LANE), F32),
            vmem((8, LANE), F32),
            vmem((8, LANE), F32),
            vmem((atoms // 8, 2, 8, WIDE), F32),
            vmem((atoms // 8, 2, 8, WIDE), F32),
            vmem((kinds, slots, WIDE), F32),
            vmem((kinds, slots, WIDE), F32),
            vmem((owners, own_rows, WIDE), F32),
            vmem((n_ga, own_rows, WIDE), F32),
            vmem((n_ga - 1, own_rows, WIDE), F32),
            vmem((n_ga - 1, own_rows, WIDE), F32),
            vmem((8, LANE), F32),
            vmem((3, group, 8, LANE), F32),
            dma((11,)),
            dma((CHUNKS,)),
            dma(()),
            dma(()),
            dma(()),
            dma((CHUNKS,)),
            dma((CHUNKS,)),
            dma((2,)),
            dma((2, n_ga)),
            dma((2, n_ga - 1)),
            dma((3 * group - 1,)),
            dma((3, group)),
        ],
        compiler_params=pltpu.CompilerParams(
            collective_id=0, has_side_effects=True, vmem_limit_bytes=60 * 1024 * 1024
        ),
    )(*args)


def solution(mesh):
    in_specs = (
        P("image", "band", None, "ga"),
        P("image", "band"),
        P(None, None, "ga"),
        P(None, "ga"),
        P(),
        P(),
        P(),
        P("image", None, None),
        P("image"),
        P("image", None, None),
        P(),
        P(),
        P(),
        P("image"),
    )
    out_specs = (P("image", None, None), P("image"))

    def run(*args):
        with jax.sharding.use_abstract_mesh(mesh.abstract_mesh):
            return jax.shard_map(
                per_device, mesh=mesh, in_specs=in_specs, out_specs=out_specs, check_vma=False
            )(*args)

    return run
```

```python
import functools

import jax
import jax.numpy as jnp
from jax import lax
from jax.experimental import pallas as pl
from jax.experimental.pallas import tpu as pltpu
from jax.sharding import PartitionSpec as P

SPRING = 5.0
SIN_HALF = (4.442882834139934, -7.308241153900935, 3.6062889473068847, -0.8457635292167789, 0.10920561914186756)
COS_HALF = (-1.414213496558818, 6.978850987079544, -5.739461141869309, 1.8835627683448501, -0.31069768559559485)
ROUNDER = 12582912.0
LANE = 128
WIDE = 256
CHUNKS = 8
MESH = pl.DeviceIdType.MESH
F32 = jnp.float32
BF16 = jnp.bfloat16


def horner(coefs, z):
    total = coefs[-1] * z + coefs[-2]
    for coef in coefs[-3::-1]:
        total = total * z + coef
    return total


def cos_and_minus_sin(phases):
    turns = phases * 0.15915494309189535
    r = turns - ((turns + ROUNDER) - ROUNDER)
    z = r * r
    half_sin = r * horner(SIN_HALF, z)
    return (1.0 - half_sin * half_sin, half_sin * horner(COS_HALF, z))


def iota(shape, dim):
    return lax.broadcasted_iota(jnp.int32, shape, dim)


def column(row, start, rows):
    n = row.shape[1]
    here = iota((rows, n), 1) == iota((rows, n), 0) + start
    return jnp.sum(jnp.where(here, row, 0.0), axis=1, keepdims=True)


def row_of(col, start):
    rows = col.shape[0]
    here = iota((rows, LANE), 1) == iota((rows, LANE), 0) + start
    return jnp.sum(jnp.where(here, col, 0.0), axis=0, keepdims=True)


def total(x):
    return jnp.sum(jnp.sum(x, axis=1, keepdims=True), axis=0, keepdims=True)


def kernel(
    w_hbm, occ_hbm, ff_hbm, g_hbm, spec_hbm, count_hbm, coup_hbm, pos_hbm, erest_hbm, frest_hbm,
    endp_hbm, ende_hbm, climb_hbm, kind_hbm,
    force_out, energy_out,
    raw_other, raw_own, w_send, w_all, ff, g, pos, coup, occ, erest, frest, endp, ende,
    spec, count, climb, kind,
    pos_wide, live, strength, occ_part, occ_peer, rad_a, rad_b, trig_a, trig_b,
    part, part_peer, z_send, z_recv, msg, msgs,
    small_sem, other_sem, own_sem, ff_sem, g_sem, w_send_sem, w_recv_sem, occ_sem,
    part_sems, z_sems, msg_send_sem, msg_recv_sem,
):
    image, band, ga = (lax.axis_index(a) for a in ("image", "band", "ga"))
    n_image, n_band, n_ga = (lax.axis_size(a) for a in ("image", "band", "ga"))
    group = n_band * n_ga
    side = lax.rem(band, 2)
    peer = band + 1 - 2 * side
    bands = w_hbm.shape[0]
    blocks, tiles = raw_own.shape[0], raw_own.shape[1]
    species, slots = coup.shape
    atoms = pos.shape[2]
    half_len = ff.shape[2]
    n_wide = half_len // WIDE
    step_tiles = tiles // CHUNKS
    n_own = z_send.shape[0]
    own_rows = z_send.shape[1]
    own_atoms = own_rows // slots
    first_own = (n_ga - n_own) // 2
    n_groups = atoms // 8

    small = [
        (occ_hbm, occ), (coup_hbm, coup), (pos_hbm, pos), (erest_hbm, erest), (frest_hbm, frest), (endp_hbm, endp),
        (ende_hbm, ende), (spec_hbm, spec), (count_hbm, count), (climb_hbm, climb), (kind_hbm, kind),
    ]
    small = [pltpu.make_async_copy(a, b, small_sem.at[i]) for i, (a, b) in enumerate(small)]

    def wave_copies(raw, which, c, count, sem):
        at = which * tiles + c * count
        return [
            pltpu.make_async_copy(
                w_hbm.at[n, pl.ds(at, count)],
                raw.at[n // 8, pl.ds(c * count, count), pl.ds(2 * (n % 8), 2), :],
                sem,
            )
            for n in range(bands)
        ]

    def start_other(c):
        for copy in wave_copies(raw_other, 1 - side, c, step_tiles, other_sem.at[c]):
            copy.start()

    mine = pl.ds(pl.multiple_of(side * half_len, WIDE), half_len)
    ff_copy = pltpu.make_async_copy(ff_hbm.at[:, :, mine], ff, ff_sem)
    g_copy = pltpu.make_async_copy(g_hbm.at[:, mine], g, g_sem)
    barrier = pltpu.get_barrier_semaphore()
    for d_image in (0, 1, n_image - 1):
        for d_band in range(n_band):
            for d_ga in range(n_ga):
                if (d_image, d_band, d_ga) != (0, 0, 0):
                    there = (
                        lax.rem(image + d_image, n_image), lax.rem(band + d_band, n_band), lax.rem(ga + d_ga, n_ga)
                    )
                    pl.semaphore_signal(barrier, inc=1, device_id=there, device_id_type=MESH)

    start_other(0)
    for copy in small:
        copy.start()
    start_other(1)

    for c in range(2, CHUNKS):
        start_other(c)
    g_copy.start()
    own_copies = wave_copies(raw_own, side, 0, tiles, own_sem)
    for copy in own_copies:
        copy.start()
    ff_copy.start()

    for copy in small:
        copy.wait()
    for c in range(3):
        for j in range(n_groups):
            pos_wide[c, 8 * j : 8 * j + 8, :] = jnp.broadcast_to(column(pos[c], 8 * j, 8), (8, LANE))
    for s in range(species):
        alive = (iota((slots, LANE), 0) < count[s]).astype(F32)
        live[s] = alive
        strength[s] = alive * column(coup[s : s + 1, :], 0, slots)
    lanes = iota((1, LANE), 1)
    here = lax.rem(lanes // bands, 2) == side
    occ_part[...] = jnp.broadcast_to(jnp.where(here, jnp.concatenate([occ[...]] * (LANE // bands), axis=1), 0.0), (8, LANE))

    def wave_push(c):
        at = pl.ds(c * step_tiles, step_tiles)
        return pltpu.make_async_remote_copy(
            src_ref=w_send.at[:, at], dst_ref=w_all.at[side, :, at],
            send_sem=w_send_sem.at[c], recv_sem=w_recv_sem.at[c],
            device_id={"band": peer}, device_id_type=MESH,
        )

    def wave_arrival(c):
        at = pl.ds(c * step_tiles, step_tiles)
        return pltpu.make_async_remote_copy(
            src_ref=w_send.at[:, at], dst_ref=w_all.at[1 - side, :, at],
            send_sem=w_send_sem.at[c], recv_sem=w_recv_sem.at[c],
            device_id={"band": peer}, device_id_type=MESH,
        )

    occ_push = pltpu.make_async_remote_copy(
        src_ref=occ_part, dst_ref=occ_peer, send_sem=occ_sem.at[0], recv_sem=occ_sem.at[1],
        device_id={"band": peer}, device_id_type=MESH,
    )

    def widen_other(c):
        def one(t, carry):
            at = c * step_tiles + t
            for b in range(blocks):
                w_send[b, at] = raw_other[b, at].astype(F32)
            return carry

        lax.fori_loop(0, step_tiles, one, 0, unroll=8)

    for c in range(CHUNKS):
        for copy in wave_copies(raw_other, 1 - side, c, step_tiles, other_sem.at[c]):
            copy.wait()
        widen_other(c)
        if c == 0:
            pl.semaphore_wait(barrier, 3 * group - 1)
        wave_push(c).start()
    occ_push.start()

    for copy in own_copies:
        copy.wait()

    def widen_own(t, carry):
        for b in range(blocks):
            w_all[side, b, t] = raw_own[b, t].astype(F32)
        return carry

    lax.fori_loop(0, tiles, widen_own, 0, unroll=8)
    g_copy.wait()
    ff_copy.wait()

    def g_rows(at):
        return [jnp.broadcast_to(g[c : c + 1, at], (8, at.size)) for c in range(3)]

    def span(k, t):
        return pl.ds(pl.multiple_of(k * WIDE + t * LANE, LANE), LANE)

    def radial(k, rad):
        for t in range(WIDE // LANE):
            for s in range(species):
                rad[s, t] = ff[s, :, span(k, t)] * live[s]

    def waves_of_atoms(k, trig, j):
        rows = slice(8 * j, 8 * j + 8)
        for t in range(WIDE // LANE):
            gs = g_rows(span(k, t))
            phases = pos_wide[0, rows, :] * gs[0]
            phases = phases + pos_wide[1, rows, :] * gs[1]
            phases = phases + pos_wide[2, rows, :] * gs[2]
            cosine, minus_sine = cos_and_minus_sin(phases)
            trig[j, 0, t] = cosine
            trig[j, 1, t] = minus_sine

    def stage(k):
        at = pl.ds(pl.multiple_of(k * WIDE, WIDE), WIDE)
        gs = g_rows(at)

        def rows(uv):
            pieces = []
            for s in range(2):
                for b in range(blocks):
                    pieces.append(jnp.concatenate(
                        [w_all[s, b, 2 * k + t, pl.ds(uv, 8, stride=2), :] for t in range(WIDE // LANE)], axis=1))
            return pieces

        u, v = rows(0), rows(1)
        real = list(u)
        imag = list(v)
        for c in range(3):
            minus = -gs[c]
            real += [minus * x for x in v]
            imag += [gs[c] * x for x in u]
        pltpu.matmul_push_rhs(jnp.concatenate(real, axis=0), 0, 0, transpose=True)
        pltpu.matmul_push_rhs(jnp.concatenate(imag, axis=0), 0, 1, transpose=True)

    def projector(rad, trig, j):
        pieces = ([], [])
        for i in range(8):
            kind_of = spec[8 * j + i]
            factors = [rad[kind_of, t] for t in range(WIDE // LANE)]
            for q in range(2):
                pieces[q].append(jnp.concatenate(
                    [factors[t] * trig[j, q, t, i : i + 1, :] for t in range(WIDE // LANE)], axis=1))
        return [jnp.concatenate(pieces[q], axis=0) for q in range(2)]

    def multiply(lhs, accs, j):
        for q in range(2):
            pltpu.matmul_acc_lhs(accs[q][j], lhs[q], load_staged_rhs=0 if j == 0 else None)

    def with_accumulators(*refs):
        accs = (refs[:n_groups], refs[n_groups:])
        for ref in refs:
            pltpu.matmul_pop(ref)

        def wide_tile(k, now, later):
            after, second = jnp.minimum(k + 1, n_wide - 1), jnp.minimum(k + 2, n_wide - 1)
            rad, trig = now
            radial(after, later[0])
            for j in range(n_groups):
                multiply(projector(rad, trig, j), accs, j)
                if j == 0:
                    stage(after)
                waves_of_atoms(second, trig, j)

        radial(0, rad_a)
        for j in range(n_groups):
            waves_of_atoms(0, trig_a, j)
            waves_of_atoms(1, trig_b, j)
        wave_arrival(0).wait_recv()
        stage(0)
        per_chunk = n_wide // CHUNKS

        def pair(i, carry):
            k = 2 * i

            @pl.when((lax.rem(k + 2, per_chunk) == 0) & (k + 2 < n_wide))
            def _():
                wave_arrival((k + 2) // per_chunk).wait_recv()

            wide_tile(k, (rad_a, trig_a), (rad_b, trig_b))
            wide_tile(k + 1, (rad_b, trig_b), (rad_a, trig_a))
            return carry

        lax.fori_loop(0, n_wide // 2, pair, 0)
        for j in range(n_groups):
            sums = 2.0 * (pltpu.matmul_pop(accs[0][j]) + pltpu.matmul_pop(accs[1][j]))
            part[j * 8 * slots : (j + 1) * 8 * slots, :] = sums
        zeros = jnp.zeros((8 * slots, WIDE), F32)
        for q in range(2):
            pltpu.matmul_acc_lhs(accs[q][0], zeros, load_staged_rhs=0)
            pltpu.matmul_pop(accs[q][0])

    pl.run_scoped(
        with_accumulators,
        *[pltpu.ACC(q)((8 * slots, WIDE), F32) for q in range(2) for _ in range(n_groups)],
    )

    def block(of_side, q):
        return pl.ds(pl.multiple_of((of_side * n_own + q) * own_rows, own_rows), own_rows)

    def pair_push(q):
        return pltpu.make_async_remote_copy(
            src_ref=part.at[block(1 - side, q)], dst_ref=part_peer.at[q],
            send_sem=part_sems.at[0, q], recv_sem=part_sems.at[1, q],
            device_id={"band": peer}, device_id_type=MESH,
        )

    def z_push(q):
        there = first_own + q
        return pltpu.make_async_remote_copy(
            src_ref=z_send.at[q], dst_ref=z_recv.at[ga],
            send_sem=z_sems.at[0, q], recv_sem=z_sems.at[1, ga],
            device_id={"ga": there}, device_id_type=MESH,
        )

    def z_arrival(sender):
        return pltpu.make_async_remote_copy(
            src_ref=z_send.at[0], dst_ref=z_recv.at[sender],
            send_sem=z_sems.at[0, 0], recv_sem=z_sems.at[1, sender],
            device_id={"band": peer}, device_id_type=MESH,
        )

    in_upper = (ga >= first_own + n_own // 2).astype(jnp.int32)
    order = [q * in_upper + (n_own - 1 - q) * (1 - in_upper) for q in range(n_own)]
    is_owner = (ga >= first_own) & (ga < first_own + n_own)
    for q in order:
        pair_push(q).start()
    for q in order:
        pair_push(q).wait_recv()
        z_send[q] = part[block(side, q), :] + part_peer[q]

        @pl.when(ga != first_own + q)
        def _():
            z_push(q).start()

    occ_push.wait()
    weights = occ_part[0:1, :] + occ_peer[0:1, :]
    place_own = jnp.clip(ga - first_own, 0, n_own - 1)
    group_own = n_band * n_own
    slot = band * n_own + place_own
    here_pos = jnp.concatenate([pos[:, 0, :], jnp.zeros((3, LANE - atoms), F32)], axis=1)

    def own_message():
        for d in range(1, n_ga):
            z_arrival(lax.rem(ga + d, n_ga)).wait_recv()
        sums = z_send[place_own]
        for d in range(1, n_ga):
            sums = sums + z_recv[lax.rem(ga + d, n_ga)]
        first = (side * n_own + place_own) * own_atoms
        low = iota((slots, LANE), 1) < LANE // 2
        rows_0, rows_1 = [], []
        for i in range(own_atoms):
            rows = slice(i * slots, (i + 1) * slots)
            left, right = sums[rows, :LANE], sums[rows, LANE:]
            becp = jnp.where(low, left, pltpu.roll(left, LANE // 2, 1))
            weighted = becp * weights * strength[spec[first + i]]
            rows_0.append(jnp.sum(weighted * left, axis=0, keepdims=True))
            rows_1.append(jnp.sum(weighted * right, axis=0, keepdims=True))
        rows_0, rows_1 = jnp.concatenate(rows_0, axis=0), jnp.concatenate(rows_1, axis=0)
        low = iota((own_atoms, LANE), 1) < LANE // 2
        cols = [
            jnp.sum(jnp.where(low == is_low, x, 0.0), axis=1, keepdims=True)
            for x, is_low in ((rows_0, True), (rows_0, False), (rows_1, True), (rows_1, False))
        ]
        energy_part = jnp.broadcast_to(jnp.sum(cols[0], axis=0, keepdims=True), (1, LANE))
        force_part = [-2.0 * row_of(col, first) for col in cols[1:]]
        rest = jnp.full((1, LANE), erest[0], F32)
        return jnp.concatenate([energy_part] + force_part + [rest, here_pos], axis=0)

    def padded(x):
        return jnp.concatenate([x, jnp.zeros((x.shape[0], LANE - x.shape[1]), F32)], axis=1)

    def message_pushes():
        pushes = []
        for place, d_image in ((1, 0), (0, 1), (2, n_image - 1)):
            for d_band in range(n_band):
                for d_ga in range(n_ga):
                    if (d_image, d_band, d_ga) != (0, 0, 0):
                        there = (
                            lax.rem(image + d_image, n_image), lax.rem(band + d_band, n_band), lax.rem(ga + d_ga, n_ga)
                        )
                        pushes.append(pltpu.make_async_remote_copy(
                            src_ref=msg, dst_ref=msgs.at[place, slot],
                            send_sem=msg_send_sem.at[len(pushes)], recv_sem=msg_recv_sem.at[place, slot],
                            device_id=there, device_id_type=MESH,
                        ))
        return pushes

    @pl.when(is_owner)
    def _():
        message = own_message()
        msg[...] = message
        msgs[1, slot] = message
        for push in message_pushes():
            push.start()

    for place in (1, 0, 2):
        for sender in range(group_own):
            arrival = pltpu.make_async_remote_copy(
                src_ref=msg, dst_ref=msgs.at[place, sender],
                send_sem=msg_send_sem.at[0], recv_sem=msg_recv_sem.at[place, sender],
                device_id=(image, peer, ga), device_id_type=MESH,
            )
            if place == 1:

                @pl.when(jnp.logical_not(is_owner & (slot == sender)))
                def _():
                    arrival.wait_recv()

            else:
                arrival.wait_recv()

    def gathered(place):
        out = msgs[place, 0]
        first_msg = out
        for s in range(1, group_own):
            out = out + msgs[place, s]
        return first_msg[4:5, 0:1] + out[0:1, 0:1], out[1:4, :], first_msg[5:8, :]

    energy, force_nl, _ = gathered(1)
    prev_energy, _, prev_pos = gathered(0)
    next_energy, _, next_pos = gathered(2)
    ends = [padded(endp[:, s, :]) for s in range(2)]
    at_start, at_end = image == 0, image == n_image - 1
    prev_pos = jnp.where(jnp.full((3, LANE), at_start), ends[0], prev_pos)
    next_pos = jnp.where(jnp.full((3, LANE), at_end), ends[1], next_pos)
    prev_energy = jnp.where(jnp.full((1, 1), at_start), jnp.full((1, 1), ende[0], F32), prev_energy)
    next_energy = jnp.where(jnp.full((1, 1), at_end), jnp.full((1, 1), ende[1], F32), next_energy)
    force = padded(frest[:, 0, :]) + force_nl

    to_next = next_pos - here_pos
    from_prev = here_pos - prev_pos
    rise_next = jnp.abs(next_energy - energy)
    rise_prev = jnp.abs(prev_energy - energy)
    larger = jnp.maximum(rise_next, rise_prev)
    smaller = jnp.minimum(rise_next, rise_prev)
    rising = next_energy > prev_energy
    weight_next = 1.0 + jnp.where(rising, larger, smaller)
    weight_prev = 1.0 + jnp.where(rising, smaller, larger)
    stiff_next = SPRING * (1.0 + 1.0 / (1.0 + jnp.exp(-0.5 * (next_energy + energy))))
    stiff_prev = SPRING * (1.0 + 1.0 / (1.0 + jnp.exp(-0.5 * (prev_energy + energy))))
    length_next = jnp.sqrt(total(to_next * to_next) + 1.0)
    length_prev = jnp.sqrt(total(from_prev * from_prev) + 1.0)
    upwind = weight_next * to_next + weight_prev * from_prev
    forward = to_next / length_next
    backward = from_prev / length_prev
    rule = jnp.full((3, LANE), kind[0], jnp.int32)
    tangent = jnp.where(
        rule == 0, upwind, jnp.where(rule == 1, forward + backward, jnp.where(rule == 2, forward, backward))
    )
    unit = tangent / jnp.sqrt(total(tangent * tangent) + 1.0)
    along = total(force * unit)
    climbing = force - 2.0 * along * unit
    regular = force - along * unit + (stiff_next * length_next - stiff_prev * length_prev) * unit
    is_climb = jnp.full((3, LANE), climb[0], jnp.int32) == image
    result = jnp.where(is_climb, climbing, regular)
    for c in range(3):
        force_out[c] = result[c : c + 1, :atoms]
    energy_out[...] = energy

    for c in range(CHUNKS):
        wave_push(c).wait_send()
    for q in range(n_own):
        pair_push(q).wait_send()

        @pl.when(ga != first_own + q)
        def _():
            z_push(q).wait_send()

    @pl.when(is_owner)
    def _():
        for push in message_pushes():
            push.wait_send()


def per_device(
    wave_coeffs, occupation, form_factor, g_vectors, species, proj_count, coupling, positions, energy_rest,
    force_rest, end_positions, end_energy, climb_index, tangent_kind,
):
    _, bands, _, length = wave_coeffs.shape
    kinds, slots, _ = form_factor.shape
    atoms = species.shape[0]
    n_band, n_ga = lax.axis_size("band"), lax.axis_size("ga")
    waves = wave_coeffs[0].reshape(bands, 2, length // LANE, LANE).transpose(0, 2, 1, 3)
    blocks = bands // 8
    tiles = length // (2 * LANE)
    half_len = length // 2
    n_own = min(n_ga, 2)
    own_rows = atoms * slots // (2 * n_own)
    group = n_band * n_ga
    positions, force_rest, end_positions = (x.transpose(1, 0, 2) for x in (positions, force_rest, end_positions))
    args = (
        waves, occupation, form_factor, g_vectors, species, proj_count, coupling, positions, energy_rest,
        force_rest, end_positions, end_energy, climb_index, tangent_kind,
    )
    vmem, smem, dma = pltpu.VMEM, pltpu.SMEM, pltpu.SemaphoreType.DMA
    force, energy = pl.pallas_call(
        kernel,
        in_specs=[pl.BlockSpec(memory_space=pltpu.HBM)] * len(args),
        out_specs=[pl.BlockSpec(memory_space=pltpu.VMEM)] * 2,
        out_shape=[jax.ShapeDtypeStruct(force_rest.shape, F32), jax.ShapeDtypeStruct((1, 1), F32)],
        scratch_shapes=[
            vmem((blocks, tiles, 16, LANE), BF16),
            vmem((blocks, tiles, 16, LANE), BF16),
            vmem((blocks, tiles, 16, LANE), F32),
            vmem((2, blocks, tiles, 16, LANE), F32),
            vmem((kinds, slots, half_len), F32),
            vmem((3, half_len), F32),
            vmem(positions.shape, F32),
            vmem(coupling.shape, F32),
            vmem(occupation.shape, F32),
            smem(energy_rest.shape, F32),
            vmem(force_rest.shape, F32),
            vmem(end_positions.shape, F32),
            smem(end_energy.shape, F32),
            smem(species.shape, jnp.int32),
            smem(proj_count.shape, jnp.int32),
            smem(climb_index.shape, jnp.int32),
            smem(tangent_kind.shape, jnp.int32),
            vmem((3, atoms, LANE), F32),
            vmem((kinds, slots, LANE), F32),
            vmem((kinds, slots, LANE), F32),
            vmem((8, LANE), F32),
            vmem((8, LANE), F32),
            vmem((kinds, 4, 8, LANE), F32),
            vmem((kinds, 4, 8, LANE), F32),
            vmem((atoms // 8, 2, WIDE // LANE, 8, LANE), F32),
            vmem((atoms // 8, 2, WIDE // LANE, 8, LANE), F32),
            vmem((atoms * slots, WIDE), F32),
            vmem((n_own, own_rows, WIDE), F32),
            vmem((n_own, own_rows, WIDE), F32),
            vmem((n_ga, own_rows, WIDE), F32),
            vmem((8, LANE), F32),
            vmem((3, n_band * n_own, 8, LANE), F32),
            dma((11,)),
            dma((CHUNKS,)),
            dma(()),
            dma(()),
            dma(()),
            dma((CHUNKS,)),
            dma((CHUNKS,)),
            dma((2,)),
            dma((2, n_own)),
            dma((2, n_ga)),
            dma((3 * group - 1,)),
            dma((3, n_band * n_own)),
        ],
        compiler_params=pltpu.CompilerParams(
            collective_id=0, has_side_effects=True, vmem_limit_bytes=60 * 1024 * 1024
        ),
    )(*args)
    return force.transpose(1, 0, 2), energy.reshape(1)


def solution(mesh):
    in_specs = (
        P("image", "band", None, "ga"),
        P("image", "band"),
        P(None, None, "ga"),
        P(None, "ga"),
        P(),
        P(),
        P(),
        P("image", None, None),
        P("image"),
        P("image", None, None),
        P(),
        P(),
        P(),
        P("image"),
    )
    out_specs = (P("image", None, None), P("image"))

    def run(*args):
        with jax.sharding.use_abstract_mesh(mesh.abstract_mesh):
            return jax.shard_map(
                per_device, mesh=mesh, in_specs=in_specs, out_specs=out_specs, check_vma=False
            )(*args)

    return run
```

```python
import functools

import jax
import jax.numpy as jnp
from jax import lax
from jax.experimental import pallas as pl
from jax.experimental.pallas import tpu as pltpu
from jax.sharding import PartitionSpec as P

SPRING = 5.0
SIN_HALF = (4.442882834139934, -7.308241153900935, 3.6062889473068847, -0.8457635292167789, 0.10920561914186756)
COS_HALF = (-1.414213496558818, 6.978850987079544, -5.739461141869309, 1.8835627683448501, -0.31069768559559485)
ROUNDER = 12582912.0
LANE = 128
WIDE = 256
CHUNKS = 8
PUSHES = 16
MESH = pl.DeviceIdType.MESH
F32 = jnp.float32
BF16 = jnp.bfloat16


def horner(coefs, z):
    total = coefs[-1] * z + coefs[-2]
    for coef in coefs[-3::-1]:
        total = total * z + coef
    return total


def cos_and_minus_sin(phases):
    turns = phases * 0.15915494309189535
    r = turns - ((turns + ROUNDER) - ROUNDER)
    z = r * r
    half_sin = r * horner(SIN_HALF, z)
    return (1.0 - half_sin * half_sin, half_sin * horner(COS_HALF, z))


def iota(shape, dim):
    return lax.broadcasted_iota(jnp.int32, shape, dim)


def column(row, start, rows):
    n = row.shape[1]
    here = iota((rows, n), 1) == iota((rows, n), 0) + start
    return jnp.sum(jnp.where(here, row, 0.0), axis=1, keepdims=True)


def row_of(col, start):
    rows = col.shape[0]
    here = iota((rows, LANE), 1) == iota((rows, LANE), 0) + start
    return jnp.sum(jnp.where(here, col, 0.0), axis=0, keepdims=True)


def total(x):
    return jnp.sum(jnp.sum(x, axis=1, keepdims=True), axis=0, keepdims=True)


def kernel(
    w_hbm, occ_hbm, ff_hbm, g_hbm, spec_hbm, count_hbm, coup_hbm, pos_hbm, erest_hbm, frest_hbm,
    endp_hbm, ende_hbm, climb_hbm, kind_hbm,
    force_out, energy_out,
    raw_other, raw_own, w_send, w_all, ff, g, pos, coup, occ, erest, frest, endp, ende,
    spec, count, climb, kind,
    pos_wide, live, strength, occ_part, occ_peer, rad_a, rad_b, trig_a, trig_b,
    part, part_peer, z_send, z_recv, msg, msgs,
    small_sem, other_sem, own_sem, ff_sem, g_sem, w_send_sem, w_recv_sem, occ_sem,
    part_sems, z_sems, msg_send_sem, msg_recv_sem,
):
    image, band, ga = (lax.axis_index(a) for a in ("image", "band", "ga"))
    n_image, n_band, n_ga = (lax.axis_size(a) for a in ("image", "band", "ga"))
    group = n_band * n_ga
    side = lax.rem(band, 2)
    peer = band + 1 - 2 * side
    bands = w_hbm.shape[0]
    blocks, tiles = raw_own.shape[0], raw_own.shape[1]
    species, slots = coup.shape
    atoms = pos.shape[2]
    half_len = ff.shape[2]
    n_wide = half_len // WIDE
    step_tiles = tiles // CHUNKS
    push_tiles = tiles // PUSHES
    split = PUSHES // CHUNKS
    n_own = z_send.shape[0]
    own_rows = z_send.shape[1]
    own_atoms = own_rows // slots
    first_own = (n_ga - n_own) // 2
    n_groups = atoms // 8

    small = [
        (occ_hbm, occ), (coup_hbm, coup), (pos_hbm, pos), (erest_hbm, erest), (frest_hbm, frest), (endp_hbm, endp),
        (ende_hbm, ende), (spec_hbm, spec), (count_hbm, count), (climb_hbm, climb), (kind_hbm, kind),
    ]
    small = [pltpu.make_async_copy(a, b, small_sem.at[i]) for i, (a, b) in enumerate(small)]

    def wave_copies(raw, which, c, count, sem):
        at = which * tiles + c * count
        return [
            pltpu.make_async_copy(
                w_hbm.at[n, pl.ds(at, count)],
                raw.at[n // 8, pl.ds(c * count, count), pl.ds(2 * (n % 8), 2), :],
                sem,
            )
            for n in range(bands)
        ]

    def start_other(c):
        for copy in wave_copies(raw_other, 1 - side, c, step_tiles, other_sem.at[c]):
            copy.start()

    mine = pl.ds(pl.multiple_of(side * half_len, WIDE), half_len)
    ff_copy = pltpu.make_async_copy(ff_hbm.at[:, :, mine], ff, ff_sem)
    g_copy = pltpu.make_async_copy(g_hbm.at[:, mine], g, g_sem)
    barrier = pltpu.get_barrier_semaphore()
    for d_image in (0, 1, n_image - 1):
        for d_band in range(n_band):
            for d_ga in range(n_ga):
                if (d_image, d_band, d_ga) != (0, 0, 0):
                    there = (
                        lax.rem(image + d_image, n_image), lax.rem(band + d_band, n_band), lax.rem(ga + d_ga, n_ga)
                    )
                    pl.semaphore_signal(barrier, inc=1, device_id=there, device_id_type=MESH)

    start_other(0)
    for copy in small:
        copy.start()
    start_other(1)

    for c in range(2, CHUNKS):
        start_other(c)
    g_copy.start()
    own_copies = wave_copies(raw_own, side, 0, tiles, own_sem)
    for copy in own_copies:
        copy.start()
    ff_copy.start()

    for copy in small:
        copy.wait()
    for c in range(3):
        for j in range(n_groups):
            pos_wide[c, 8 * j : 8 * j + 8, :] = jnp.broadcast_to(column(pos[c], 8 * j, 8), (8, LANE))
    for s in range(species):
        alive = (iota((slots, LANE), 0) < count[s]).astype(F32)
        live[s] = alive
        strength[s] = alive * column(coup[s : s + 1, :], 0, slots)
    lanes = iota((1, LANE), 1)
    here = lax.rem(lanes // bands, 2) == side
    occ_part[...] = jnp.broadcast_to(jnp.where(here, jnp.concatenate([occ[...]] * (LANE // bands), axis=1), 0.0), (8, LANE))

    def wave_push(c):
        at = pl.ds(c * push_tiles, push_tiles)
        return pltpu.make_async_remote_copy(
            src_ref=w_send.at[:, at], dst_ref=w_all.at[side, :, at],
            send_sem=w_send_sem.at[c], recv_sem=w_recv_sem.at[c],
            device_id={"band": peer}, device_id_type=MESH,
        )

    def wave_arrival(c):
        at = pl.ds(c * push_tiles, push_tiles)
        return pltpu.make_async_remote_copy(
            src_ref=w_send.at[:, at], dst_ref=w_all.at[1 - side, :, at],
            send_sem=w_send_sem.at[c], recv_sem=w_recv_sem.at[c],
            device_id={"band": peer}, device_id_type=MESH,
        )

    occ_push = pltpu.make_async_remote_copy(
        src_ref=occ_part, dst_ref=occ_peer, send_sem=occ_sem.at[0], recv_sem=occ_sem.at[1],
        device_id={"band": peer}, device_id_type=MESH,
    )

    def widen_other(c):
        def one(t, carry):
            at = c * push_tiles + t
            for b in range(blocks):
                w_send[b, at] = raw_other[b, at].astype(F32)
            return carry

        lax.fori_loop(0, push_tiles, one, 0, unroll=8)

    for c in range(CHUNKS):
        for copy in wave_copies(raw_other, 1 - side, c, step_tiles, other_sem.at[c]):
            copy.wait()
        for p in range(c * split, (c + 1) * split):
            widen_other(p)
            if p == 0:
                pl.semaphore_wait(barrier, 3 * group - 1)
            wave_push(p).start()
    occ_push.start()

    for copy in own_copies:
        copy.wait()

    def widen_own(t, carry):
        for b in range(blocks):
            w_all[side, b, t] = raw_own[b, t].astype(F32)
        return carry

    lax.fori_loop(0, tiles, widen_own, 0, unroll=8)
    g_copy.wait()
    ff_copy.wait()

    def g_rows(at):
        return [jnp.broadcast_to(g[c : c + 1, at], (8, at.size)) for c in range(3)]

    def span(k, t):
        return pl.ds(pl.multiple_of(k * WIDE + t * LANE, LANE), LANE)

    def radial(k, rad):
        for t in range(WIDE // LANE):
            for s in range(species):
                rad[s, t] = ff[s, :, span(k, t)] * live[s]

    def waves_of_atoms(k, trig, j):
        rows = slice(8 * j, 8 * j + 8)
        for t in range(WIDE // LANE):
            gs = g_rows(span(k, t))
            phases = pos_wide[0, rows, :] * gs[0]
            phases = phases + pos_wide[1, rows, :] * gs[1]
            phases = phases + pos_wide[2, rows, :] * gs[2]
            cosine, minus_sine = cos_and_minus_sin(phases)
            trig[j, 0, t] = cosine
            trig[j, 1, t] = minus_sine

    def stage(k):
        at = pl.ds(pl.multiple_of(k * WIDE, WIDE), WIDE)
        gs = g_rows(at)

        def rows(uv):
            pieces = []
            for s in range(2):
                for b in range(blocks):
                    pieces.append(jnp.concatenate(
                        [w_all[s, b, 2 * k + t, pl.ds(uv, 8, stride=2), :] for t in range(WIDE // LANE)], axis=1))
            return pieces

        u, v = rows(0), rows(1)
        real = list(u)
        imag = list(v)
        for c in range(3):
            minus = -gs[c]
            real += [minus * x for x in v]
            imag += [gs[c] * x for x in u]
        pltpu.matmul_push_rhs(jnp.concatenate(real, axis=0), 0, 0, transpose=True)
        pltpu.matmul_push_rhs(jnp.concatenate(imag, axis=0), 0, 1, transpose=True)

    def projector(rad, trig, j):
        pieces = ([], [])
        for i in range(8):
            kind_of = spec[8 * j + i]
            factors = [rad[kind_of, t] for t in range(WIDE // LANE)]
            for q in range(2):
                pieces[q].append(jnp.concatenate(
                    [factors[t] * trig[j, q, t, i : i + 1, :] for t in range(WIDE // LANE)], axis=1))
        return [jnp.concatenate(pieces[q], axis=0) for q in range(2)]

    def multiply(lhs, accs, j):
        for q in range(2):
            pltpu.matmul_acc_lhs(accs[q][j], lhs[q], load_staged_rhs=0 if j == 0 else None)

    def with_accumulators(*refs):
        accs = (refs[:n_groups], refs[n_groups:])
        for ref in refs:
            pltpu.matmul_pop(ref)

        def wide_tile(k, now, later):
            after, second = jnp.minimum(k + 1, n_wide - 1), jnp.minimum(k + 2, n_wide - 1)
            rad, trig = now
            radial(after, later[0])
            for j in range(n_groups):
                multiply(projector(rad, trig, j), accs, j)
                if j == 0:
                    stage(after)
                waves_of_atoms(second, trig, j)

        radial(0, rad_a)
        for j in range(n_groups):
            waves_of_atoms(0, trig_a, j)
            waves_of_atoms(1, trig_b, j)
        wave_arrival(0).wait_recv()
        stage(0)
        per_chunk = n_wide // PUSHES

        def pair(i, carry):
            k = 2 * i

            @pl.when((lax.rem(k + 2, per_chunk) == 0) & (k + 2 < n_wide))
            def _():
                wave_arrival((k + 2) // per_chunk).wait_recv()

            wide_tile(k, (rad_a, trig_a), (rad_b, trig_b))
            wide_tile(k + 1, (rad_b, trig_b), (rad_a, trig_a))
            return carry

        lax.fori_loop(0, n_wide // 2, pair, 0)
        for j in range(n_groups):
            sums = 2.0 * (pltpu.matmul_pop(accs[0][j]) + pltpu.matmul_pop(accs[1][j]))
            part[j * 8 * slots : (j + 1) * 8 * slots, :] = sums
        zeros = jnp.zeros((8 * slots, WIDE), F32)
        for q in range(2):
            pltpu.matmul_acc_lhs(accs[q][0], zeros, load_staged_rhs=0)
            pltpu.matmul_pop(accs[q][0])

    pl.run_scoped(
        with_accumulators,
        *[pltpu.ACC(q)((8 * slots, WIDE), F32) for q in range(2) for _ in range(n_groups)],
    )

    def block(of_side, q):
        return pl.ds(pl.multiple_of((of_side * n_own + q) * own_rows, own_rows), own_rows)

    def pair_push(q):
        return pltpu.make_async_remote_copy(
            src_ref=part.at[block(1 - side, q)], dst_ref=part_peer.at[q],
            send_sem=part_sems.at[0, q], recv_sem=part_sems.at[1, q],
            device_id={"band": peer}, device_id_type=MESH,
        )

    def z_push(q):
        there = first_own + q
        return pltpu.make_async_remote_copy(
            src_ref=z_send.at[q], dst_ref=z_recv.at[ga],
            send_sem=z_sems.at[0, q], recv_sem=z_sems.at[1, ga],
            device_id={"ga": there}, device_id_type=MESH,
        )

    def z_arrival(sender):
        return pltpu.make_async_remote_copy(
            src_ref=z_send.at[0], dst_ref=z_recv.at[sender],
            send_sem=z_sems.at[0, 0], recv_sem=z_sems.at[1, sender],
            device_id={"band": peer}, device_id_type=MESH,
        )

    in_upper = (ga >= first_own + n_own // 2).astype(jnp.int32)
    order = [q * in_upper + (n_own - 1 - q) * (1 - in_upper) for q in range(n_own)]
    is_owner = (ga >= first_own) & (ga < first_own + n_own)
    for q in order:
        pair_push(q).start()
    for q in order:
        pair_push(q).wait_recv()
        z_send[q] = part[block(side, q), :] + part_peer[q]

        @pl.when(ga != first_own + q)
        def _():
            z_push(q).start()

    occ_push.wait()
    weights = occ_part[0:1, :] + occ_peer[0:1, :]
    place_own = jnp.clip(ga - first_own, 0, n_own - 1)
    group_own = n_band * n_own
    slot = band * n_own + place_own
    here_pos = jnp.concatenate([pos[:, 0, :], jnp.zeros((3, LANE - atoms), F32)], axis=1)

    def own_message():
        for d in range(1, n_ga):
            z_arrival(lax.rem(ga + d, n_ga)).wait_recv()
        sums = z_send[place_own]
        for d in range(1, n_ga):
            sums = sums + z_recv[lax.rem(ga + d, n_ga)]
        first = (side * n_own + place_own) * own_atoms
        low = iota((slots, LANE), 1) < LANE // 2
        rows_0, rows_1 = [], []
        for i in range(own_atoms):
            rows = slice(i * slots, (i + 1) * slots)
            left, right = sums[rows, :LANE], sums[rows, LANE:]
            becp = jnp.where(low, left, pltpu.roll(left, LANE // 2, 1))
            weighted = becp * weights * strength[spec[first + i]]
            rows_0.append(jnp.sum(weighted * left, axis=0, keepdims=True))
            rows_1.append(jnp.sum(weighted * right, axis=0, keepdims=True))
        rows_0, rows_1 = jnp.concatenate(rows_0, axis=0), jnp.concatenate(rows_1, axis=0)
        low = iota((own_atoms, LANE), 1) < LANE // 2
        cols = [
            jnp.sum(jnp.where(low == is_low, x, 0.0), axis=1, keepdims=True)
            for x, is_low in ((rows_0, True), (rows_0, False), (rows_1, True), (rows_1, False))
        ]
        energy_part = jnp.broadcast_to(jnp.sum(cols[0], axis=0, keepdims=True), (1, LANE))
        force_part = [-2.0 * row_of(col, first) for col in cols[1:]]
        rest = jnp.full((1, LANE), erest[0], F32)
        return jnp.concatenate([energy_part] + force_part + [rest, here_pos], axis=0)

    def padded(x):
        return jnp.concatenate([x, jnp.zeros((x.shape[0], LANE - x.shape[1]), F32)], axis=1)

    def message_pushes():
        pushes = []
        for place, d_image in ((1, 0), (0, 1), (2, n_image - 1)):
            for d_band in range(n_band):
                for d_ga in range(n_ga):
                    if (d_image, d_band, d_ga) != (0, 0, 0):
                        there = (
                            lax.rem(image + d_image, n_image), lax.rem(band + d_band, n_band), lax.rem(ga + d_ga, n_ga)
                        )
                        pushes.append(pltpu.make_async_remote_copy(
                            src_ref=msg, dst_ref=msgs.at[place, slot],
                            send_sem=msg_send_sem.at[len(pushes)], recv_sem=msg_recv_sem.at[place, slot],
                            device_id=there, device_id_type=MESH,
                        ))
        return pushes

    @pl.when(is_owner)
    def _():
        message = own_message()
        msg[...] = message
        msgs[1, slot] = message
        for push in message_pushes():
            push.start()

    for place in (1, 0, 2):
        for sender in range(group_own):
            arrival = pltpu.make_async_remote_copy(
                src_ref=msg, dst_ref=msgs.at[place, sender],
                send_sem=msg_send_sem.at[0], recv_sem=msg_recv_sem.at[place, sender],
                device_id=(image, peer, ga), device_id_type=MESH,
            )
            if place == 1:

                @pl.when(jnp.logical_not(is_owner & (slot == sender)))
                def _():
                    arrival.wait_recv()

            else:
                arrival.wait_recv()

    def gathered(place):
        out = msgs[place, 0]
        first_msg = out
        for s in range(1, group_own):
            out = out + msgs[place, s]
        return first_msg[4:5, 0:1] + out[0:1, 0:1], out[1:4, :], first_msg[5:8, :]

    energy, force_nl, _ = gathered(1)
    prev_energy, _, prev_pos = gathered(0)
    next_energy, _, next_pos = gathered(2)
    ends = [padded(endp[:, s, :]) for s in range(2)]
    at_start, at_end = image == 0, image == n_image - 1
    prev_pos = jnp.where(jnp.full((3, LANE), at_start), ends[0], prev_pos)
    next_pos = jnp.where(jnp.full((3, LANE), at_end), ends[1], next_pos)
    prev_energy = jnp.where(jnp.full((1, 1), at_start), jnp.full((1, 1), ende[0], F32), prev_energy)
    next_energy = jnp.where(jnp.full((1, 1), at_end), jnp.full((1, 1), ende[1], F32), next_energy)
    force = padded(frest[:, 0, :]) + force_nl

    to_next = next_pos - here_pos
    from_prev = here_pos - prev_pos
    rise_next = jnp.abs(next_energy - energy)
    rise_prev = jnp.abs(prev_energy - energy)
    larger = jnp.maximum(rise_next, rise_prev)
    smaller = jnp.minimum(rise_next, rise_prev)
    rising = next_energy > prev_energy
    weight_next = 1.0 + jnp.where(rising, larger, smaller)
    weight_prev = 1.0 + jnp.where(rising, smaller, larger)
    stiff_next = SPRING * (1.0 + 1.0 / (1.0 + jnp.exp(-0.5 * (next_energy + energy))))
    stiff_prev = SPRING * (1.0 + 1.0 / (1.0 + jnp.exp(-0.5 * (prev_energy + energy))))
    length_next = jnp.sqrt(total(to_next * to_next) + 1.0)
    length_prev = jnp.sqrt(total(from_prev * from_prev) + 1.0)
    upwind = weight_next * to_next + weight_prev * from_prev
    forward = to_next / length_next
    backward = from_prev / length_prev
    rule = jnp.full((3, LANE), kind[0], jnp.int32)
    tangent = jnp.where(
        rule == 0, upwind, jnp.where(rule == 1, forward + backward, jnp.where(rule == 2, forward, backward))
    )
    unit = tangent / jnp.sqrt(total(tangent * tangent) + 1.0)
    along = total(force * unit)
    climbing = force - 2.0 * along * unit
    regular = force - along * unit + (stiff_next * length_next - stiff_prev * length_prev) * unit
    is_climb = jnp.full((3, LANE), climb[0], jnp.int32) == image
    result = jnp.where(is_climb, climbing, regular)
    for c in range(3):
        force_out[c] = result[c : c + 1, :atoms]
    energy_out[...] = energy

    for c in range(PUSHES):
        wave_push(c).wait_send()
    for q in range(n_own):
        pair_push(q).wait_send()

        @pl.when(ga != first_own + q)
        def _():
            z_push(q).wait_send()

    @pl.when(is_owner)
    def _():
        for push in message_pushes():
            push.wait_send()


def per_device(
    wave_coeffs, occupation, form_factor, g_vectors, species, proj_count, coupling, positions, energy_rest,
    force_rest, end_positions, end_energy, climb_index, tangent_kind,
):
    _, bands, _, length = wave_coeffs.shape
    kinds, slots, _ = form_factor.shape
    atoms = species.shape[0]
    n_band, n_ga = lax.axis_size("band"), lax.axis_size("ga")
    waves = wave_coeffs[0].reshape(bands, 2, length // LANE, LANE).transpose(0, 2, 1, 3)
    blocks = bands // 8
    tiles = length // (2 * LANE)
    half_len = length // 2
    n_own = min(n_ga, 2)
    own_rows = atoms * slots // (2 * n_own)
    group = n_band * n_ga
    positions, force_rest, end_positions = (x.transpose(1, 0, 2) for x in (positions, force_rest, end_positions))
    args = (
        waves, occupation, form_factor, g_vectors, species, proj_count, coupling, positions, energy_rest,
        force_rest, end_positions, end_energy, climb_index, tangent_kind,
    )
    vmem, smem, dma = pltpu.VMEM, pltpu.SMEM, pltpu.SemaphoreType.DMA
    force, energy = pl.pallas_call(
        kernel,
        in_specs=[pl.BlockSpec(memory_space=pltpu.HBM)] * len(args),
        out_specs=[pl.BlockSpec(memory_space=pltpu.VMEM)] * 2,
        out_shape=[jax.ShapeDtypeStruct(force_rest.shape, F32), jax.ShapeDtypeStruct((1, 1), F32)],
        scratch_shapes=[
            vmem((blocks, tiles, 16, LANE), BF16),
            vmem((blocks, tiles, 16, LANE), BF16),
            vmem((blocks, tiles, 16, LANE), F32),
            vmem((2, blocks, tiles, 16, LANE), F32),
            vmem((kinds, slots, half_len), F32),
            vmem((3, half_len), F32),
            vmem(positions.shape, F32),
            vmem(coupling.shape, F32),
            vmem(occupation.shape, F32),
            smem(energy_rest.shape, F32),
            vmem(force_rest.shape, F32),
            vmem(end_positions.shape, F32),
            smem(end_energy.shape, F32),
            smem(species.shape, jnp.int32),
            smem(proj_count.shape, jnp.int32),
            smem(climb_index.shape, jnp.int32),
            smem(tangent_kind.shape, jnp.int32),
            vmem((3, atoms, LANE), F32),
            vmem((kinds, slots, LANE), F32),
            vmem((kinds, slots, LANE), F32),
            vmem((8, LANE), F32),
            vmem((8, LANE), F32),
            vmem((kinds, 4, 8, LANE), F32),
            vmem((kinds, 4, 8, LANE), F32),
            vmem((atoms // 8, 2, WIDE // LANE, 8, LANE), F32),
            vmem((atoms // 8, 2, WIDE // LANE, 8, LANE), F32),
            vmem((atoms * slots, WIDE), F32),
            vmem((n_own, own_rows, WIDE), F32),
            vmem((n_own, own_rows, WIDE), F32),
            vmem((n_ga, own_rows, WIDE), F32),
            vmem((8, LANE), F32),
            vmem((3, n_band * n_own, 8, LANE), F32),
            dma((11,)),
            dma((CHUNKS,)),
            dma(()),
            dma(()),
            dma(()),
            dma((PUSHES,)),
            dma((PUSHES,)),
            dma((2,)),
            dma((2, n_own)),
            dma((2, n_ga)),
            dma((3 * group - 1,)),
            dma((3, n_band * n_own)),
        ],
        compiler_params=pltpu.CompilerParams(
            collective_id=0, has_side_effects=True, vmem_limit_bytes=60 * 1024 * 1024
        ),
    )(*args)
    return force.transpose(1, 0, 2), energy.reshape(1)


def solution(mesh):
    in_specs = (
        P("image", "band", None, "ga"),
        P("image", "band"),
        P(None, None, "ga"),
        P(None, "ga"),
        P(),
        P(),
        P(),
        P("image", None, None),
        P("image"),
        P("image", None, None),
        P(),
        P(),
        P(),
        P("image"),
    )
    out_specs = (P("image", None, None), P("image"))

    def run(*args):
        with jax.sharding.use_abstract_mesh(mesh.abstract_mesh):
            return jax.shard_map(
                per_device, mesh=mesh, in_specs=in_specs, out_specs=out_specs, check_vma=False
            )(*args)

    return run
```
